32 devices in a mesh: rows: 4 (over y, x), mp: 8 (over z, core).
Axes of the slice: x: 2, y: 2, z: 4, core: 2. Of those that a mesh axis runs over, the one named last changes fastest.
Arguments:
- tokens: bfloat16 [512, 6144], P('rows', 'mp'), may hold values from -8 to 8
- norm_gain: float32 [6144], replicated, may hold values from 0.25 to 1.75
- hidden_bias: float32 [24576], P('mp'), may hold values from -3 to 3
- weight_in: bfloat16 [6144, 24576], P('rows', 'mp'), may hold values from -0.078125 to 0.078125
- weight_out: bfloat16 [24576, 6144], P('mp', 'rows'), may hold values from -0.0546875 to 0.0546875
Outputs:
- updated: bfloat16 [512, 6144], P('rows', 'mp')
The draws below stay inside these ranges and needn't reach their ends.
All inputs are finite; a program needn't handle non-finite values.
Results may differ from the reference program's by a relative error of at most 0.0041.
Values may be sent and summed in bfloat16 or wider, within the bound.
A program may use at most 128 MiB of HBM per device.

```python
import jax
import jax.numpy as jnp
from jax import lax

D = 6144
FF = 24576
TOKENS = 512


def raised(array, own_key, source, target, blocks, factor):
    owner, partner = [(jnp.arange(array.shape[position]) // (array.shape[position] // blocks)).reshape([-1 if axis == position else 1 for axis in range(array.ndim)]) for position in (source, target)]
    chosen = jax.random.permutation(own_key, blocks)[partner]
    strong = (owner == chosen) | (owner == (partner + blocks // 2) % blocks)
    return jnp.where(strong, factor * array, array)


def block_scale(own_key, extent, cuts, smallest, high):
    factor_of = 1.0
    for dim, blocks in cuts:
        heights = jax.random.uniform(jax.random.fold_in(jax.random.fold_in(own_key, 6), dim), (blocks,), jnp.float32, smallest / len(cuts), high / len(cuts))
        factor_of = factor_of * jnp.repeat(jnp.exp(heights), extent[dim] // blocks).reshape((-1,) + (1,) * (len(extent) - 1 - dim))
    return factor_of


def gaussian(own_key, extent, spread, limit, split=(), dtype=jnp.bfloat16):
    array = spread * jax.random.normal(own_key, extent, jnp.float32)
    if split:
        array = array * block_scale(own_key, extent, split, -0.22, 0.18)
    return jnp.clip(array, -limit, limit).astype(dtype)


def heavy_noise(stream_key, extent, spread, reach, shards, heavy, kind=jnp.bfloat16):
    array = spread * jax.random.normal(stream_key, extent, jnp.float32)
    if shards:
        array = array * block_scale(stream_key, extent, shards, -0.22, 0.18)
    return jnp.clip(raised(array, jax.random.fold_in(stream_key, 3), *heavy), -reach, reach).astype(kind)


def setup_inputs(seed: int = 0) -> dict:
    streams_of = jax.random.split(jax.random.key(seed), 6)
    return {
        "tokens": heavy_noise(streams_of[0], (TOKENS, D), 1.0, 8.0, ((0, 4), (1, 8)), (1, 0, 8, 2.0)),
        "norm_gain": jnp.clip(1.0 + 0.15 * jax.random.normal(streams_of[1], (D,), jnp.float32), 0.25, 1.75),
        "hidden_bias": gaussian(streams_of[2], (FF,), 0.5, 3.0, ((0, 8),), jnp.float32),
        "weight_in": gaussian(streams_of[3], (D, FF), D ** -0.5, 0.078125, ((0, 4), (1, 8))),
        "weight_out": heavy_noise(streams_of[4], (FF, D), FF ** -0.5, 0.0546875, ((0, 8), (1, 4)), (0, 1, 8, 2.0)),
    }


floor_value = 0.1

def normalize(as_float, moment_sum, square_sum, gain, width):
    row_mean = moment_sum / width
    row_var = jnp.maximum(square_sum / width - row_mean * row_mean, 0.0)
    inverse = lax.rsqrt(row_var + floor_value)
    return ((as_float - row_mean[:, None]) * inverse[:, None] * gain[None, :]).astype(jnp.bfloat16)

def reference(tokens, norm_gain, hidden_bias, weight_in, weight_out):
    as_float = tokens.astype(jnp.float32)
    normed = normalize(as_float, lax.optimization_barrier(jnp.sum(as_float, axis=1)), lax.optimization_barrier(jnp.sum(as_float * as_float, axis=1)), norm_gain, D)
    preact = jnp.dot(normed, weight_in, preferred_element_type=jnp.float32) + hidden_bias[None, :]
    hidden = jax.nn.gelu(preact, approximate=False).astype(jnp.bfloat16)
    branch = jnp.dot(hidden, weight_out, preferred_element_type=jnp.float32)
    return (as_float + branch).astype(jnp.bfloat16)
```

```python
import functools

import jax
import jax.numpy as jnp
from jax import lax
from jax.experimental import pallas as pl
from jax.experimental.pallas import tpu as pltpu
from jax.sharding import PartitionSpec as P

MESH = pl.DeviceIdType.MESH
F32 = jnp.float32
BF16 = jnp.bfloat16
floor_value = 0.1
CHUNKS = 4


def gelu(x):
    return 0.5 * x * (1.0 + lax.erf(x * 0.7071067811865476))


def kernel(
    R, M, K, D, tok, gain, bias, win_hbm, wout_hbm, out, win, wout, xs, nx, stat, pbuf, r1, r2, qbuf, hid,
    osend, osib, oown, zlo, zhi, zsend, fsend, fbuf, wsem,
    s_src, s_dn, s_up, s_sib, r_x, r_xs, s_st, r_st, s_r1, r_r1, s_r2, r_r2, s_ag, r_ag, s_os, r_os, s_z, r_zl, r_zh,
    s_f, r_f,
):
    r = lax.axis_index("rows")
    m = lax.axis_index("mp")
    Z = M // 2
    z, c = m // 2, m % 2
    sib = 2 * z + 1 - c
    rows = tok.shape[0] // K
    width = tok.shape[1]
    half = win.shape[1] // 2
    rx, ry, rd = r + 1 - 2 * (r % 2), (r + 2) % 4, 3 - r
    first, second = (rx, ry), (ry, rx)
    peers = (rx, ry, rd)

    pltpu.make_async_copy(win_hbm, win, wsem.at[0]).start()
    pltpu.make_async_copy(wout_hbm, wout, wsem.at[1]).start()

    barrier = pltpu.get_barrier_semaphore()
    for peer in peers:
        pl.semaphore_signal(barrier, inc=1, device_id=(peer, m), device_id_type=MESH)
    pl.semaphore_signal(barrier, inc=1, device_id=(r, sib), device_id_type=MESH)

    @pl.when(z > 0)
    def _():
        pl.semaphore_signal(barrier, inc=1, device_id=(r, m - 2), device_id_type=MESH)

    @pl.when(z < Z - 1)
    def _():
        pl.semaphore_signal(barrier, inc=1, device_id=(r, m + 2), device_id_type=MESH)

    pl.semaphore_wait(barrier, 4 + jnp.where(z > 0, 1, 0) + jnp.where(z < Z - 1, 1, 0))

    def remote(src, dst, ssem, rsem, row, col):
        return pltpu.make_async_remote_copy(
            src_ref=src, dst_ref=dst, send_sem=ssem, recv_sem=rsem, device_id=(row, col), device_id_type=MESH
        )

    def c_src(k):
        return remote(tok.at[pl.ds(k * rows, rows)], xs.at[k, r, c], s_src.at[k], r_x.at[k, r], z, m)

    def c_x(k, t, col, ssem):
        return remote(xs.at[k, t, c], xs.at[k, t, c], ssem.at[k, t], r_x.at[k, t], r, col)

    def c_sib(k, t):
        return remote(xs.at[k, t, c], xs.at[k, t, c], s_sib.at[k, t], r_xs.at[k, t], r, sib)

    def w_sib(k, t):
        return remote(xs.at[k, t, 1 - c], xs.at[k, t, 1 - c], s_sib.at[k, t], r_xs.at[k, t], r, sib)

    def c_st(k, i):
        return remote(stat.at[k, r], stat.at[k, r], s_st.at[k, i], r_st.at[k, r], peers[i], m)

    def w_st(k, i):
        return remote(stat.at[k, peers[i]], stat.at[k, peers[i]], s_st.at[k, i], r_st.at[k, peers[i]], peers[i], m)

    def c_r1(k, h, i):
        tile = (first[h], rd)[i]
        return remote(pbuf.at[k, h, tile], r1.at[k, h, i], s_r1.at[k, h, i], r_r1.at[k, h, i], first[h], m)

    def c_r2(k, h):
        return remote(qbuf.at[k, h], r2.at[k, h], s_r2.at[k, h], r_r2.at[k, h], second[h], m)

    def c_ag(k, h, i):
        tile = (r, r, second[h])[i]
        to = (second[h], first[h], first[h])[i]
        return remote(hid.at[k, h, tile], hid.at[k, h, tile], s_ag.at[k, h, i], r_ag.at[k, h, tile], to, m)

    def w_ag(k, h, tile):
        return remote(hid.at[k, h, tile], hid.at[k, h, tile], s_ag.at[k, h, 0], r_ag.at[k, h, tile], first[h], m)

    def c_os(k):
        return remote(osend.at[k], osib.at[k], s_os.at[k], r_os.at[k], r, sib)

    def c_zl(k, t, col):
        return remote(zsend.at[k, t], zlo.at[k, t], s_z.at[k, t], r_zl.at[k, t], r, col)

    def c_zh(k, t, col):
        return remote(zsend.at[k, t], zhi.at[k, t], s_z.at[k, t], r_zh.at[k, t], r, col)

    def c_f(k, t):
        return remote(fsend.at[k, t], fbuf.at[k], s_f.at[k, t], r_f.at[k], t, m)

    home = z == r
    has_dn = (z <= r) & (z > 0)
    has_up = (z >= r) & (z < Z - 1)

    @pl.when(home)
    def _():
        for k in range(K):
            xs[k, r, c] = tok[k * rows:(k + 1) * rows]

    @pl.when(jnp.logical_not(home))
    def _():
        for k in range(K):
            c_src(k).start()

    def stage_a(k):
        for t in range(R):
            @pl.when(jnp.logical_not(home & (r == t)))
            def _():
                c_x(k, t, sib, s_dn).wait_recv()

            @pl.when(has_dn)
            def _():
                c_x(k, t, m - 2, s_dn).start()

            @pl.when(has_up)
            def _():
                c_x(k, t, m + 2, s_up).start()

            c_sib(k, t).start()

    def chunk_x(k, cc):
        return xs[k, :, cc].astype(F32).reshape(R * rows, width)

    def stage_s(k):
        for t in range(R):
            w_sib(k, t).wait_recv()
        s1 = 0.0
        s2 = 0.0
        for cc in range(2):
            x = chunk_x(k, cc)
            s1 = s1 + jnp.sum(x, axis=1, keepdims=True)
            s2 = s2 + jnp.sum(x * x, axis=1, keepdims=True)
        lane = lax.broadcasted_iota(jnp.int32, (R * rows, 128), 1)
        both = jnp.where(lane == 0, s1, s2)
        stat[k, r] = both.T[0:8]
        for i in range(3):
            c_st(k, i).start()

    def stage_m1(k):
        for i in range(3):
            w_st(k, i).wait_recv()
        tot = (stat[k, 0] + stat[k, 1]) + (stat[k, 2] + stat[k, 3])
        mean = tot[0:1] / D
        var = jnp.maximum(tot[1:2] / D - mean * mean, 0.0)
        inv = lax.rsqrt(var + floor_value)
        sub = lax.broadcasted_iota(jnp.int32, (128, R * rows), 0)
        cols = jnp.where(sub == 0, mean, inv).T
        mean_c, inv_c = cols[:, 0:1], cols[:, 1:2]
        for cc in range(2):
            nx[cc] = ((chunk_x(k, cc) - mean_c) * inv_c * gain[2 * r + cc]).astype(BF16)

        @pl.when(k == 0)
        def _():
            pltpu.make_async_copy(win_hbm, win, wsem.at[0]).wait()

        tile = half // 2

        for h in range(2):
            def col(j, _):
                at = pl.multiple_of(j * tile, 128)
                wat = pl.multiple_of(h * half + j * tile, 128)
                acc = jnp.dot(nx[0], win[0:width, pl.ds(wat, tile)], preferred_element_type=F32)
                acc += jnp.dot(nx[1], win[width:2 * width, pl.ds(wat, tile)], preferred_element_type=F32)
                pbuf[k, h, :, :, pl.ds(at, tile)] = acc.astype(BF16).reshape(R, rows, tile)
                return 0

            lax.fori_loop(0, 2, col, 0)
            c_r1(k, h, 1).start()
            c_r1(k, h, 0).start()

    def stage_b1(k):
        for h in range(2):
            c_r1(k, h, 1).wait_recv()
            qbuf[k, h] = (pbuf[k, h, second[h]].astype(F32) + r1[k, h, 1].astype(F32)).astype(BF16)
            c_r2(k, h).start()

    def stage_b2(k):
        for h in range(2):
            c_r1(k, h, 0).wait_recv()
            c_r2(k, h).wait_recv()
            pre = pbuf[k, h, r].astype(F32) + r1[k, h, 0].astype(F32) + r2[k, h].astype(F32)
            pre = pre + bias[0:1, h * half:(h + 1) * half]
            hid[k, h, r] = gelu(pre).astype(BF16)
            c_ag(k, h, 0).start()
            c_ag(k, h, 1).start()

    def stage_b3(k):
        for h in range(2):
            w_ag(k, h, second[h]).wait_recv()
            c_ag(k, h, 2).start()

    def stage_b4(k):
        for h in range(2):
            w_ag(k, h, first[h]).wait_recv()
            w_ag(k, h, rd).wait_recv()

        @pl.when(k == 0)
        def _():
            pltpu.make_async_copy(wout_hbm, wout, wsem.at[1]).wait()

        def product(cc):
            at = pl.multiple_of(cc * width, 128)
            acc = None
            for h in range(2):
                a = hid[k, h].reshape(R * rows, half)
                part = jnp.dot(a, wout[h * half:(h + 1) * half, pl.ds(at, width)], preferred_element_type=F32)
                acc = part if acc is None else acc + part
            return acc.reshape(R, rows, width)

        osend[k] = product(1 - c).astype(BF16)
        c_os(k).start()
        oown[k] = product(c)

    def stage_c(k):
        c_os(k).wait_recv()
        for t in range(R):
            oown[k, t] = oown[k, t] + osib[k, t].astype(F32)

            @pl.when(has_dn)
            def _():
                c_zl(k, t, sib).wait_recv()
                oown[k, t] = oown[k, t] + zlo[k, t].astype(F32)

            @pl.when(has_up)
            def _():
                c_zh(k, t, sib).wait_recv()
                oown[k, t] = oown[k, t] + zhi[k, t].astype(F32)

            @pl.when(home)
            def _():
                done = (xs[k, t, c].astype(F32) + oown[k, t]).astype(BF16)

                @pl.when(r == t)
                def _():
                    fbuf[k] = done

                @pl.when(r != t)
                def _():
                    fsend[k, t] = done
                    c_f(k, t).start()

            @pl.when(jnp.logical_not(home))
            def _():
                zsend[k, t] = oown[k, t].astype(BF16)

            @pl.when(z < r)
            def _():
                c_zl(k, t, m + 2).start()

            @pl.when(z > r)
            def _():
                c_zh(k, t, m - 2).start()

    def at_chunk(k, fn):
        @pl.when((k >= 0) & (k < K))
        def _():
            fn(k)

    stage_a(0)
    stage_s(0)
    behind = jnp.where(z < r, z, jnp.where(z > r, Z - 1 - z, jnp.maximum(z, Z - 1 - z)))

    def step(t, _):
        at_chunk(t, stage_m1)
        at_chunk(t + 1, stage_a)
        at_chunk(t + 1, stage_s)
        at_chunk(t - 1, stage_b1)
        at_chunk(t - 2, stage_b3)
        at_chunk(t - 1, stage_b2)
        at_chunk(t - 2, stage_b4)
        at_chunk(t - 2 - behind, stage_c)
        return 0

    lax.fori_loop(0, K + 2 + Z - 1, step, 0)

    def drain(k, _):
        for t in range(R):
            @pl.when(has_dn)
            def _():
                c_x(k, t, sib, s_dn).wait_send()

            @pl.when(has_up)
            def _():
                c_x(k, t, sib, s_up).wait_send()

            c_sib(k, t).wait_send()

            @pl.when(home & (r != t))
            def _():
                c_f(k, t).wait_send()

            @pl.when(jnp.logical_not(home))
            def _():
                c_zl(k, t, sib).wait_send()

        @pl.when(jnp.logical_not(home))
        def _():
            c_src(k).wait_send()
            c_f(k, rx).wait_recv()

        for i in range(3):
            c_st(k, i).wait_send()
        for h in range(2):
            c_r1(k, h, 0).wait_send()
            c_r1(k, h, 1).wait_send()
            c_r2(k, h).wait_send()
            for i in range(3):
                c_ag(k, h, i).wait_send()
        c_os(k).wait_send()
        return 0

    lax.fori_loop(0, K, drain, 0)
    for k in range(K):
        out[k * rows:(k + 1) * rows] = fbuf[k]


def fused(tokens, norm_gain, hidden_bias, weight_in, weight_out, R, M, D, K):
    height, width = tokens.shape
    depth, ff = weight_in.shape
    rows, half = height // K, ff // 2
    V = pltpu.VMEM
    S = pltpu.SemaphoreType.DMA
    vm = pl.BlockSpec(memory_space=pltpu.VMEM)
    hbm = pl.BlockSpec(memory_space=pltpu.HBM)
    return pl.pallas_call(
        functools.partial(kernel, R, M, K, D),
        out_shape=jax.ShapeDtypeStruct(tokens.shape, BF16),
        in_specs=[vm, vm, vm, hbm, hbm],
        out_specs=vm,
        scratch_shapes=[
            V(weight_in.shape, BF16), V(weight_out.shape, BF16),
            V((K, R, 2, rows, width), BF16), V((2, R * rows, width), BF16), V((K, R, 8, R * rows), F32),
            V((K, 2, R, rows, half), BF16), V((K, 2, 2, rows, half), BF16), V((K, 2, rows, half), BF16),
            V((K, 2, rows, half), BF16), V((K, 2, R, rows, half), BF16),
            V((K, R, rows, width), BF16), V((K, R, rows, width), BF16), V((K, R, rows, width), F32),
            V((K, R, rows, width), BF16), V((K, R, rows, width), BF16), V((K, R, rows, width), BF16),
            V((K, R, rows, width), BF16), V((K, rows, width), BF16), S((2,)),
            S((K,)), S((K, R)), S((K, R)), S((K, R)), S((K, R)), S((K, R)), S((K, 3)), S((K, R)),
            S((K, 2, 2)), S((K, 2, 2)), S((K, 2)), S((K, 2)), S((K, 2, 3)), S((K, 2, R)), S((K,)), S((K,)),
            S((K, R)), S((K, R)), S((K, R)), S((K, R)), S((K,)),
        ],
        compiler_params=pltpu.CompilerParams(
            collective_id=0, has_side_effects=True, vmem_limit_bytes=60 * 1024 * 1024
        ),
    )(tokens, norm_gain.reshape(M, 1, width), hidden_bias.reshape(1, ff), weight_in, weight_out)


def plain(tokens, norm_gain, hidden_bias, weight_in, weight_out, R, M, D):
    as_float = tokens.astype(F32)
    moment_sum, square_sum = lax.psum((jnp.sum(as_float, axis=1), jnp.sum(as_float * as_float, axis=1)), "mp")
    width = tokens.shape[1]
    gain = lax.dynamic_slice_in_dim(norm_gain, lax.axis_index("mp") * width, width)
    mean = moment_sum / D
    inverse = lax.rsqrt(jnp.maximum(square_sum / D - mean * mean, 0.0) + floor_value)
    part = ((as_float - mean[:, None]) * inverse[:, None] * gain[None, :]).astype(BF16)
    normed = lax.all_gather(part, "mp", axis=1, tiled=True)
    shuffled = lax.all_to_all(normed, "rows", split_axis=1, concat_axis=0, tiled=True)
    preact = lax.psum_scatter(
        jnp.dot(shuffled, weight_in, preferred_element_type=F32), "rows", scatter_dimension=0, tiled=True
    )
    hidden = jax.nn.gelu(preact + hidden_bias[None, :], approximate=False).astype(BF16)
    hidden = lax.all_gather(hidden, "rows", axis=0, tiled=True)
    terms = jnp.dot(hidden, weight_out, preferred_element_type=F32)
    terms = lax.all_to_all(terms, "rows", split_axis=0, concat_axis=1, tiled=True)
    branch = lax.psum_scatter(terms, "mp", scatter_dimension=1, tiled=True)
    return (as_float + branch).astype(BF16)


def solution(mesh):
    R, M = mesh.shape["rows"], mesh.shape["mp"]

    def body(tokens, norm_gain, hidden_bias, weight_in, weight_out):
        D = norm_gain.shape[0]
        aligned = tokens.shape[1] % 128 == 0 and weight_in.shape[1] % 512 == 0 and tokens.shape[0] % (32 * CHUNKS) == 0
        if R == 4 and M == 2 * R and aligned:
            return fused(tokens, norm_gain, hidden_bias, weight_in, weight_out, R, M, D, CHUNKS)
        return plain(tokens, norm_gain, hidden_bias, weight_in, weight_out, R, M, D)

    return jax.shard_map(
        body,
        mesh=mesh,
        in_specs=(P("rows", "mp"), P(), P("mp"), P("rows", "mp"), P("mp", "rows")),
        out_specs=P("rows", "mp"),
        check_vma=False,
    )
```

```python
import functools

import jax
import jax.numpy as jnp
from jax import lax
from jax.experimental import pallas as pl
from jax.experimental.pallas import tpu as pltpu
from jax.sharding import PartitionSpec as P

MESH = pl.DeviceIdType.MESH
F32 = jnp.float32
BF16 = jnp.bfloat16
floor_value = 0.1
CHUNKS = 4


def gelu(x):
    return 0.5 * x * (1.0 + lax.erf(x * 0.7071067811865476))


def kernel(
    R, M, K, D, tok, gain, bias, win_hbm, wout_hbm, out, win, wout, xs, nx, stat, pbuf, r1, r2, qbuf, hid,
    osend, osib, oown, zlo, zhi, zsend, fsend, fbuf, wsem,
    s_src, s_dn, s_up, s_sib, r_x, r_xs, s_st, r_st, s_r1, r_r1, s_r2, r_r2, s_ag, r_ag, s_os, r_os, s_z, r_zl, r_zh,
    s_f, r_f,
):
    r = lax.axis_index("rows")
    m = lax.axis_index("mp")
    Z = M // 2
    z, c = m // 2, m % 2
    sib = 2 * z + 1 - c
    rows = tok.shape[0] // K
    width = tok.shape[1]
    half = win.shape[1] // 2
    rx, ry, rd = r + 1 - 2 * (r % 2), (r + 2) % 4, 3 - r
    first, second = (rx, ry), (ry, rx)
    peers = (rx, ry, rd)

    pltpu.make_async_copy(win_hbm, win, wsem.at[0]).start()
    pltpu.make_async_copy(wout_hbm, wout, wsem.at[1]).start()

    barrier = pltpu.get_barrier_semaphore()
    for peer in peers:
        pl.semaphore_signal(barrier, inc=1, device_id=(peer, m), device_id_type=MESH)
    pl.semaphore_signal(barrier, inc=1, device_id=(r, sib), device_id_type=MESH)

    @pl.when(z > 0)
    def _():
        pl.semaphore_signal(barrier, inc=1, device_id=(r, m - 2), device_id_type=MESH)

    @pl.when(z < Z - 1)
    def _():
        pl.semaphore_signal(barrier, inc=1, device_id=(r, m + 2), device_id_type=MESH)

    pl.semaphore_wait(barrier, 4 + jnp.where(z > 0, 1, 0) + jnp.where(z < Z - 1, 1, 0))

    def remote(src, dst, ssem, rsem, row, col):
        return pltpu.make_async_remote_copy(
            src_ref=src, dst_ref=dst, send_sem=ssem, recv_sem=rsem, device_id=(row, col), device_id_type=MESH
        )

    def c_src(k):
        return remote(tok.at[pl.ds(k * rows, rows)], xs.at[k, r, c], s_src.at[k], r_x.at[k, r], z, m)

    def c_x(k, t, col, ssem):
        return remote(xs.at[k, t, c], xs.at[k, t, c], ssem.at[k, t], r_x.at[k, t], r, col)

    def c_sib(k, t):
        return remote(xs.at[k, t, c], xs.at[k, t, c], s_sib.at[k, t], r_xs.at[k, t], r, sib)

    def w_sib(k, t):
        return remote(xs.at[k, t, 1 - c], xs.at[k, t, 1 - c], s_sib.at[k, t], r_xs.at[k, t], r, sib)

    def c_st(k, i):
        return remote(stat.at[k, r], stat.at[k, r], s_st.at[k, i], r_st.at[k, r], peers[i], m)

    def w_st(k, i):
        return remote(stat.at[k, peers[i]], stat.at[k, peers[i]], s_st.at[k, i], r_st.at[k, peers[i]], peers[i], m)

    def c_r1(k, h, i):
        tile = (first[h], rd)[i]
        return remote(pbuf.at[k, h, tile], r1.at[k, h, i], s_r1.at[k, h, i], r_r1.at[k, h, i], first[h], m)

    def c_r2(k, h):
        return remote(qbuf.at[k, h], r2.at[k, h], s_r2.at[k, h], r_r2.at[k, h], second[h], m)

    def c_ag(k, h, i):
        tile = (r, r, second[h])[i]
        to = (second[h], first[h], first[h])[i]
        return remote(hid.at[k, h, tile], hid.at[k, h, tile], s_ag.at[k, h, i], r_ag.at[k, h, tile], to, m)

    def w_ag(k, h, tile):
        return remote(hid.at[k, h, tile], hid.at[k, h, tile], s_ag.at[k, h, 0], r_ag.at[k, h, tile], first[h], m)

    def c_os(k):
        return remote(osend.at[k], osib.at[k], s_os.at[k], r_os.at[k], r, sib)

    def c_zl(k, t, col):
        return remote(zsend.at[k, t], zlo.at[k, t], s_z.at[k, t], r_zl.at[k, t], r, col)

    def c_zh(k, t, col):
        return remote(zsend.at[k, t], zhi.at[k, t], s_z.at[k, t], r_zh.at[k, t], r, col)

    def c_f(k, t):
        return remote(fsend.at[k, t], fbuf.at[k], s_f.at[k, t], r_f.at[k], t, m)

    home = z == r
    has_dn = (z <= r) & (z > 0)
    has_up = (z >= r) & (z < Z - 1)

    @pl.when(home)
    def _():
        for k in range(K):
            xs[k, r, c] = tok[k * rows:(k + 1) * rows]

    @pl.when(jnp.logical_not(home))
    def _():
        for k in range(K):
            c_src(k).start()

    def stage_a(k):
        for t in range(R):
            @pl.when(jnp.logical_not(home & (r == t)))
            def _():
                c_x(k, t, sib, s_dn).wait_recv()

            @pl.when(has_dn)
            def _():
                c_x(k, t, m - 2, s_dn).start()

            @pl.when(has_up)
            def _():
                c_x(k, t, m + 2, s_up).start()

            c_sib(k, t).start()

    def chunk_x(k, cc):
        return xs[k, :, cc].astype(F32).reshape(R * rows, width)

    def stage_s(k):
        for t in range(R):
            w_sib(k, t).wait_recv()
        s1 = 0.0
        s2 = 0.0
        for cc in range(2):
            x = chunk_x(k, cc)
            s1 = s1 + jnp.sum(x, axis=1, keepdims=True)
            s2 = s2 + jnp.sum(x * x, axis=1, keepdims=True)
        lane = lax.broadcasted_iota(jnp.int32, (R * rows, 128), 1)
        both = jnp.where(lane == 0, s1, s2)
        stat[k, r] = both.T[0:8]
        for i in range(3):
            c_st(k, i).start()

    def stage_m1(k):
        for i in range(3):
            w_st(k, i).wait_recv()
        tot = (stat[k, 0] + stat[k, 1]) + (stat[k, 2] + stat[k, 3])
        mean = tot[0:1] / D
        var = jnp.maximum(tot[1:2] / D - mean * mean, 0.0)
        inv = lax.rsqrt(var + floor_value)
        sub = lax.broadcasted_iota(jnp.int32, (128, R * rows), 0)
        cols = jnp.where(sub == 0, mean, inv).T
        mean_c, inv_c = cols[:, 0:1], cols[:, 1:2]
        for cc in range(2):
            nx[cc] = ((chunk_x(k, cc) - mean_c) * inv_c * gain[2 * r + cc]).astype(BF16)

        @pl.when(k == 0)
        def _():
            pltpu.make_async_copy(win_hbm, win, wsem.at[0]).wait()

        tile = half // 2

        for h in range(2):
            def col(j, _):
                at = pl.multiple_of(j * tile, 128)
                wat = pl.multiple_of(h * half + j * tile, 128)
                acc = jnp.dot(nx[0], win[0:width, pl.ds(wat, tile)], preferred_element_type=F32)
                acc += jnp.dot(nx[1], win[width:2 * width, pl.ds(wat, tile)], preferred_element_type=F32)
                pbuf[k, h, :, :, pl.ds(at, tile)] = acc.astype(BF16).reshape(R, rows, tile)
                return 0

            lax.fori_loop(0, 2, col, 0)
            c_r1(k, h, 1).start()
            c_r1(k, h, 0).start()

    def stage_b1(k):
        for h in range(2):
            c_r1(k, h, 1).wait_recv()
            qbuf[k, h] = (pbuf[k, h, second[h]].astype(F32) + r1[k, h, 1].astype(F32)).astype(BF16)
            c_r2(k, h).start()

    def stage_b2(k):
        for h in range(2):
            c_r1(k, h, 0).wait_recv()
            c_r2(k, h).wait_recv()
            pre = pbuf[k, h, r].astype(F32) + r1[k, h, 0].astype(F32) + r2[k, h].astype(F32)
            pre = pre + bias[0:1, h * half:(h + 1) * half]
            hid[k, h, r] = gelu(pre).astype(BF16)
            c_ag(k, h, 0).start()
            c_ag(k, h, 1).start()

    def stage_b3(k):
        for h in range(2):
            w_ag(k, h, second[h]).wait_recv()
            c_ag(k, h, 2).start()

    def stage_b4(k):
        for h in range(2):
            w_ag(k, h, first[h]).wait_recv()
            w_ag(k, h, rd).wait_recv()

        @pl.when(k == 0)
        def _():
            pltpu.make_async_copy(wout_hbm, wout, wsem.at[1]).wait()

        def product(cc):
            at = pl.multiple_of(cc * width, 128)
            acc = None
            for h in range(2):
                a = hid[k, h].reshape(R * rows, half)
                part = jnp.dot(a, wout[h * half:(h + 1) * half, pl.ds(at, width)], preferred_element_type=F32)
                acc = part if acc is None else acc + part
            return acc.reshape(R, rows, width)

        osend[k] = product(1 - c).astype(BF16)
        c_os(k).start()
        oown[k] = product(c)

    def stage_c(k):
        c_os(k).wait_recv()
        for t in range(R):
            oown[k, t] = oown[k, t] + osib[k, t].astype(F32)

            @pl.when(has_dn)
            def _():
                c_zl(k, t, sib).wait_recv()
                oown[k, t] = oown[k, t] + zlo[k, t].astype(F32)

            @pl.when(has_up)
            def _():
                c_zh(k, t, sib).wait_recv()
                oown[k, t] = oown[k, t] + zhi[k, t].astype(F32)

            @pl.when(home)
            def _():
                done = (xs[k, t, c].astype(F32) + oown[k, t]).astype(BF16)

                @pl.when(r == t)
                def _():
                    fbuf[k] = done

                @pl.when(r != t)
                def _():
                    fsend[k, t] = done
                    c_f(k, t).start()

            @pl.when(jnp.logical_not(home))
            def _():
                zsend[k, t] = oown[k, t].astype(BF16)

            @pl.when(z < r)
            def _():
                c_zl(k, t, m + 2).start()

            @pl.when(z > r)
            def _():
                c_zh(k, t, m - 2).start()

    def at_chunk(k, fn):
        @pl.when((k >= 0) & (k < K))
        def _():
            fn(k)

    behind = jnp.where(z < r, z, jnp.where(z > r, Z - 1 - z, jnp.maximum(z, Z - 1 - z)))
    lead = jnp.minimum(Z - 1 - jnp.maximum(z - r, r - z), K - 1)

    def ahead(k, _):
        stage_a(k)
        return 0

    lax.fori_loop(0, lead + 1, ahead, 0)
    stage_s(0)

    def step(t, _):
        at_chunk(t + 1 + lead, stage_a)
        at_chunk(t + 1, stage_s)
        at_chunk(t - 1, stage_b1)
        at_chunk(t, stage_m1)
        at_chunk(t - 2, stage_b3)
        at_chunk(t - 1, stage_b2)
        at_chunk(t - 2, stage_b4)
        at_chunk(t - 2 - behind, stage_c)
        return 0

    lax.fori_loop(0, K + 2 + Z - 1, step, 0)

    def drain(k, _):
        for t in range(R):
            @pl.when(has_dn)
            def _():
                c_x(k, t, sib, s_dn).wait_send()

            @pl.when(has_up)
            def _():
                c_x(k, t, sib, s_up).wait_send()

            c_sib(k, t).wait_send()

            @pl.when(home & (r != t))
            def _():
                c_f(k, t).wait_send()

            @pl.when(jnp.logical_not(home))
            def _():
                c_zl(k, t, sib).wait_send()

        @pl.when(jnp.logical_not(home))
        def _():
            c_src(k).wait_send()
            c_f(k, rx).wait_recv()

        for i in range(3):
            c_st(k, i).wait_send()
        for h in range(2):
            c_r1(k, h, 0).wait_send()
            c_r1(k, h, 1).wait_send()
            c_r2(k, h).wait_send()
            for i in range(3):
                c_ag(k, h, i).wait_send()
        c_os(k).wait_send()
        return 0

    lax.fori_loop(0, K, drain, 0)
    for k in range(K):
        out[k * rows:(k + 1) * rows] = fbuf[k]


def fused(tokens, norm_gain, hidden_bias, weight_in, weight_out, R, M, D, K):
    height, width = tokens.shape
    depth, ff = weight_in.shape
    rows, half = height // K, ff // 2
    V = pltpu.VMEM
    S = pltpu.SemaphoreType.DMA
    vm = pl.BlockSpec(memory_space=pltpu.VMEM)
    hbm = pl.BlockSpec(memory_space=pltpu.HBM)
    return pl.pallas_call(
        functools.partial(kernel, R, M, K, D),
        out_shape=jax.ShapeDtypeStruct(tokens.shape, BF16),
        in_specs=[vm, vm, vm, hbm, hbm],
        out_specs=vm,
        scratch_shapes=[
            V(weight_in.shape, BF16), V(weight_out.shape, BF16),
            V((K, R, 2, rows, width), BF16), V((2, R * rows, width), BF16), V((K, R, 8, R * rows), F32),
            V((K, 2, R, rows, half), BF16), V((K, 2, 2, rows, half), BF16), V((K, 2, rows, half), BF16),
            V((K, 2, rows, half), BF16), V((K, 2, R, rows, half), BF16),
            V((K, R, rows, width), BF16), V((K, R, rows, width), BF16), V((K, R, rows, width), F32),
            V((K, R, rows, width), BF16), V((K, R, rows, width), BF16), V((K, R, rows, width), BF16),
            V((K, R, rows, width), BF16), V((K, rows, width), BF16), S((2,)),
            S((K,)), S((K, R)), S((K, R)), S((K, R)), S((K, R)), S((K, R)), S((K, 3)), S((K, R)),
            S((K, 2, 2)), S((K, 2, 2)), S((K, 2)), S((K, 2)), S((K, 2, 3)), S((K, 2, R)), S((K,)), S((K,)),
            S((K, R)), S((K, R)), S((K, R)), S((K, R)), S((K,)),
        ],
        compiler_params=pltpu.CompilerParams(
            collective_id=0, has_side_effects=True, vmem_limit_bytes=60 * 1024 * 1024
        ),
    )(tokens, norm_gain.reshape(M, 1, width), hidden_bias.reshape(1, ff), weight_in, weight_out)


def plain(tokens, norm_gain, hidden_bias, weight_in, weight_out, R, M, D):
    as_float = tokens.astype(F32)
    moment_sum, square_sum = lax.psum((jnp.sum(as_float, axis=1), jnp.sum(as_float * as_float, axis=1)), "mp")
    width = tokens.shape[1]
    gain = lax.dynamic_slice_in_dim(norm_gain, lax.axis_index("mp") * width, width)
    mean = moment_sum / D
    inverse = lax.rsqrt(jnp.maximum(square_sum / D - mean * mean, 0.0) + floor_value)
    part = ((as_float - mean[:, None]) * inverse[:, None] * gain[None, :]).astype(BF16)
    normed = lax.all_gather(part, "mp", axis=1, tiled=True)
    shuffled = lax.all_to_all(normed, "rows", split_axis=1, concat_axis=0, tiled=True)
    preact = lax.psum_scatter(
        jnp.dot(shuffled, weight_in, preferred_element_type=F32), "rows", scatter_dimension=0, tiled=True
    )
    hidden = jax.nn.gelu(preact + hidden_bias[None, :], approximate=False).astype(BF16)
    hidden = lax.all_gather(hidden, "rows", axis=0, tiled=True)
    terms = jnp.dot(hidden, weight_out, preferred_element_type=F32)
    terms = lax.all_to_all(terms, "rows", split_axis=0, concat_axis=1, tiled=True)
    branch = lax.psum_scatter(terms, "mp", scatter_dimension=1, tiled=True)
    return (as_float + branch).astype(BF16)


def solution(mesh):
    R, M = mesh.shape["rows"], mesh.shape["mp"]

    def body(tokens, norm_gain, hidden_bias, weight_in, weight_out):
        D = norm_gain.shape[0]
        aligned = tokens.shape[1] % 128 == 0 and weight_in.shape[1] % 512 == 0 and tokens.shape[0] % (32 * CHUNKS) == 0
        if R == 4 and M == 2 * R and aligned:
            return fused(tokens, norm_gain, hidden_bias, weight_in, weight_out, R, M, D, CHUNKS)
        return plain(tokens, norm_gain, hidden_bias, weight_in, weight_out, R, M, D)

    return jax.shard_map(
        body,
        mesh=mesh,
        in_specs=(P("rows", "mp"), P(), P("mp"), P("rows", "mp"), P("mp", "rows")),
        out_specs=P("rows", "mp"),
        check_vma=False,
    )
```
